64 devices in a mesh: dp: 4 (over x, y), dcp: 16 (over z, core).
Axes of the slice: x: 2, y: 2, z: 8, core: 2. Of those that a mesh axis runs over, the one named last changes fastest.
The devices are a block of a 4x4x8 slice.
Arguments:
- q_abs: bfloat16 [32, 2, 128, 576], P('dp', None, 'dcp'), parts along dimension 0
- kv_cache: bfloat16 [32, 32, 16, 64, 576], P('dp', None, 'dcp'), parts along dimension 0
- lengths: int32 [32], P('dp'), parts along dimension 0
Outputs:
- output: bfloat16 [32, 2, 128, 512], P('dp', None, 'dcp'), parts along dimension 0
There are 4 independent parts. The reference program is written for one: setup_inputs(seed, part) draws one part's arguments, and reference() takes and returns one part's arrays. A program takes and returns all parts, laid end to end along the dimension named above; each array names one.
All inputs are finite; a program needn't handle non-finite values.
Results may differ from the reference program's by a relative error of at most 0.0063045.
Values are sent between devices in bfloat16 or wider.
A program may use at most 768 MiB of HBM per device.

```python
import math
import jax
import jax.numpy as jnp
from jax import lax

BATCH = 8
MTP = 2
HEADS = 128
LATENT = 512
ROPE = 64
NOPE = 128
ROUNDS = 32
GROUP = 16
PAGE = 64

SEQ = ROUNDS * GROUP * PAGE
WIDTH = LATENT + ROPE


def setup_inputs(seed: int = 0, part: int = 0) -> dict:
    base_key = jax.random.fold_in(jax.random.key(seed), part)
    key_qlat, key_qrope, key_cache, key_len, key_pick = jax.random.split(base_key, 5)
    lat_scale = math.sqrt(SEQ / 256.0)
    q_lat = jax.random.normal(key_qlat, (BATCH, MTP, HEADS, LATENT), jnp.float32) * (math.sqrt(1.8 * (NOPE + ROPE) / LATENT) / lat_scale)
    q_rope = jax.random.normal(key_qrope, (BATCH, MTP, HEADS, ROPE), jnp.float32) * math.sqrt(1.8 * (NOPE + ROPE) / ROPE)
    q_abs = jnp.concatenate([q_lat, q_rope], axis=-1).astype(jnp.bfloat16)
    col_scale = jnp.where(jnp.arange(WIDTH) < LATENT, lat_scale, 1.0)
    kv_cache = (jax.random.normal(key_cache, (BATCH, ROUNDS, GROUP, PAGE, WIDTH), jnp.float32) * col_scale).astype(jnp.bfloat16)
    lengths = jax.random.randint(key_len, (BATCH,), SEQ // 2, SEQ + 1, dtype=jnp.int32)
    longest = jax.random.randint(key_pick, (), 0, BATCH, dtype=jnp.int32)
    lengths = jnp.where(jnp.arange(BATCH) == longest, SEQ, lengths).astype(jnp.int32)
    return {'q_abs': q_abs, 'kv_cache': kv_cache, 'lengths': lengths}


def reference(q_abs, kv_cache, lengths):
    keys_all = kv_cache.reshape(BATCH, SEQ, WIDTH)
    score_scale = (NOPE + ROPE) ** -0.5
    positions = jnp.arange(SEQ)
    offsets = jnp.arange(MTP) - MTP

    def one_seq(seq_args):
        q_seq, key_seq, length = seq_args
        key_f = key_seq.astype(jnp.float32)
        scores = jnp.einsum('thd,sd->ths', q_seq.astype(jnp.float32), key_f) * score_scale
        last_pos = length + offsets
        visible = positions[None, :] <= last_pos[:, None]
        scores = jnp.where(visible[:, None, :], scores, -jnp.inf)
        weights = jax.nn.softmax(scores, axis=-1)
        out_seq = jnp.einsum('ths,sc->thc', weights, key_f[:, :LATENT])
        return out_seq.astype(jnp.bfloat16)

    return lax.map(one_seq, (q_abs, keys_all, lengths))
```

```python
import functools
import math

import jax
import jax.numpy as jnp
from jax import lax
from jax.experimental import pallas as pl
from jax.experimental.pallas import tpu as pltpu
from jax.sharding import PartitionSpec as P

LATENT = 512
ROPE = 64
NOPE = 128
PAGE = 64
LANES = 128
PACKED = LATENT + LANES
MESH = pl.DeviceIdType.MESH


def _lse_limbs(lse):
    hi = lse.astype(jnp.bfloat16).astype(jnp.float32)
    rest = lse - hi
    mid = rest.astype(jnp.bfloat16).astype(jnp.float32)
    low = rest - mid
    shape = lse.shape[:-1] + (LANES,)
    lane = lax.broadcasted_iota(jnp.int32, shape, len(shape) - 1)
    zero = jnp.zeros(shape, jnp.float32)
    tile = jnp.where(lane == 0, hi, jnp.where(lane == 1, mid, jnp.where(lane == 2, low, zero)))
    return tile.astype(jnp.bfloat16)


def _merge(parts):
    lses = [jnp.sum(p[:, LATENT:].astype(jnp.float32), axis=-1, keepdims=True) for p in parts]
    top = functools.reduce(jnp.maximum, lses)
    ws = [jnp.exp2(x - top) for x in lses]
    total = functools.reduce(jnp.add, ws)
    inv = 1.0 / total
    out = functools.reduce(jnp.add, [p[:, :LATENT].astype(jnp.float32) * (w * inv) for p, w in zip(parts, ws)])
    return out, top + jnp.log2(total)


def _kernel(group, toks, heads, len_ref, q_hbm, kv_hbm, o_ref, kv_buf, q_buf, p_buf, d_buf, c_buf, r_buf, s_buf, pos_ref,
            sc_ref, w_ref, kv_sem, qin_sem, ql_recv, qp_recv, q_send, qp_send, d_recv, d_send, r_recv, r_send):
    batch, keys, width = kv_buf.shape
    rows = toks * heads
    chips = group // 2
    all_rows = group * rows
    scale = (NOPE + ROPE) ** -0.5 * math.log2(math.e)
    me = lax.axis_index('dcp')
    z = lax.div(me, 2)
    core = lax.rem(me, 2)
    other = 1 - core

    def chip(off):
        return lax.rem(z + off + chips, chips)

    def dev(off):
        return chip(off) * 2 + core

    partner = z * 2 + other

    def remote(src, dst, send, recv, target):
        return pltpu.make_async_remote_copy(src_ref=src, dst_ref=dst, send_sem=send, recv_sem=recv, device_id={'dcp': target}, device_id_type=MESH)

    def sign(b):
        return 1 - 2 * lax.rem(b, 2)

    own_q = pltpu.make_async_copy(q_hbm, q_buf.at[:, core, z], qin_sem)
    own_q.start()

    def kv_copy(b):
        return pltpu.make_async_copy(kv_hbm.at[b], kv_buf.at[b], kv_sem.at[b])

    def start_kv(b, carry):
        kv_copy(b).start()
        return carry

    lax.fori_loop(0, batch, start_kv, 0)

    barrier = pltpu.get_barrier_semaphore()
    for target in (dev(-1), dev(1), partner):
        pl.semaphore_signal(barrier, inc=1, device_id={'dcp': target}, device_id_type=MESH)
    pl.semaphore_wait(barrier, 3)

    def q_desc(b, src, target, slot):
        ref = q_buf.at[b, core, src]
        return remote(ref, ref, q_send.at[b], ql_recv.at[b, slot], target)

    own_q.wait()

    def send_own(b, carry):
        q_desc(b, z, dev(1), 0).start()
        q_desc(b, z, dev(-1), 3).start()
        return carry

    lax.fori_loop(0, batch, send_own, 0)

    col = lax.broadcasted_iota(jnp.int32, (rows, keys), 1)
    tok = lax.broadcasted_iota(jnp.int32, (rows, keys), 0) // heads
    pos_ref[...] = ((col // PAGE) * group + me) * PAGE + col % PAGE - tok + toks

    def q1(b):
        q_desc(b, chip(-1), partner, 0).wait_recv()
        q_desc(b, chip(-1), dev(1), 1).start()
        q_desc(b, chip(1), partner, 3).wait_recv()
        q_desc(b, chip(1), dev(-1), 4).start()

    def q2(b):
        q_desc(b, chip(-2), partner, 1).wait_recv()
        q_desc(b, chip(-2), dev(1), 2).start()
        q_desc(b, chip(2), partner, 4).wait_recv()
        q_desc(b, chip(2), dev(-1), 5).start()

    def q3(b):
        q_desc(b, chip(-3), partner, 2).wait_recv()
        q_desc(b, chip(3), partner, 5).wait_recv()
        q_desc(b, chip(-3 * sign(b)), dev(sign(b)), 6).start()

    def qp_desc(b, side):
        ref = q_buf.at[b, side]
        return remote(ref, ref, qp_send.at[b], qp_recv.at[b], partner)

    def q4(b):
        q_desc(b, chip(4), partner, 6).wait_recv()
        qp_desc(b, core).start()

    def d_desc(b):
        return remote(p_buf.at[b, other], d_buf.at[b], d_send.at[b], d_recv.at[b], partner)

    def attend(b):
        qp_desc(b, other).wait_recv()
        kv_copy(b).wait()
        q = q_buf[b].reshape(all_rows, width)
        limit = len_ref[b]
        cap = jnp.where(pos_ref[...] <= limit, jnp.inf, -jnp.inf).astype(jnp.float32)
        block = 512
        tops = []
        for j in range(keys // block):
            ks = slice(j * block, (j + 1) * block)
            s = lax.dot_general(q, kv_buf[b, ks, :], (((1,), (1,)), ((), ())), preferred_element_type=jnp.float32)
            s = jnp.minimum(s.reshape(group, rows, block) * scale, cap[None, :, ks]).reshape(all_rows, block)
            sc_ref[:, ks] = s
            tops.append(jnp.max(s, axis=-1, keepdims=True))
        top = functools.reduce(jnp.maximum, tops)
        sums = []
        for j in range(keys // block):
            ks = slice(j * block, (j + 1) * block)
            w = jnp.exp2(sc_ref[:, ks] - top)
            sums.append(jnp.sum(w, axis=-1, keepdims=True))
            w_ref[:, ks] = w.astype(jnp.bfloat16)
        total = functools.reduce(jnp.add, sums)
        out = jnp.dot(w_ref[...], kv_buf[b, :, :LATENT], preferred_element_type=jnp.float32)
        out = (out * (1.0 / total)).astype(jnp.bfloat16)
        p_buf[b, :, :, :, :LATENT] = out.reshape(2, chips, rows, LATENT)
        p_buf[b, :, :, :, LATENT:] = _lse_limbs(top + jnp.log2(total)).reshape(2, chips, rows, LANES)
        d_desc(b).start()

    def pack(ref, part):
        out, lse = part
        ref[:, :LATENT] = out.astype(jnp.bfloat16)
        ref[:, LATENT:] = _lse_limbs(lse)

    def r_desc(b, src, slot, target):
        return remote(src, r_buf.at[b, slot], r_send.at[b], r_recv.at[b, slot], target)

    def r_wait(b, slot):
        r_desc(b, r_buf.at[b, slot], slot, partner).wait_recv()

    def o0(b):
        d_desc(b).wait_recv()
        n = chips * rows
        out, lse = _merge([p_buf[b, core].reshape(n, PACKED), d_buf[b].reshape(n, PACKED)])
        c_buf[b, :, :, :LATENT] = out.astype(jnp.bfloat16).reshape(chips, rows, LATENT)
        c_buf[b, :, :, LATENT:] = _lse_limbs(lse).reshape(chips, rows, LANES)
        r_desc(b, c_buf.at[b, chip(4)], 0, dev(sign(b))).start()
        r_desc(b, c_buf.at[b, chip(-3 * sign(b))], 4, dev(-sign(b))).start()

    def hop(b, slot, off, dst, direction):
        pack(s_buf.at[b, dst], _merge([r_buf[b, slot], c_buf[b, chip(off)]]))
        r_desc(b, s_buf.at[b, dst], slot + 1, dev(direction)).start()

    def o1(b):
        s = sign(b)
        r_wait(b, 0)
        r_wait(b, 4)
        hop(b, 0, 3 * s, 0, s)
        hop(b, 4, -2 * s, 1, -s)

    def o2(b):
        s = sign(b)
        r_wait(b, 1)
        r_wait(b, 5)
        hop(b, 1, 2 * s, 2, s)
        hop(b, 5, -s, 3, -s)

    def o3(b):
        s = sign(b)
        r_wait(b, 2)
        hop(b, 2, s, 4, s)

    def o4(b):
        r_wait(b, 3)
        r_wait(b, 6)
        out, _ = _merge([r_buf[b, 3], r_buf[b, 6], c_buf[b, z]])
        o_ref[b] = out.astype(jnp.bfloat16)

    stages = [(0, q1), (2, q2), (4, q3), (6, q4), (8, o0), (10, o1), (12, o2), (14, o3), (16, o4), (7, attend)]

    def wave(w, carry):
        for off, stage in stages:
            b = w - off

            @pl.when(jnp.logical_and(b >= 0, b < batch))
            def _(stage=stage, b=b):
                stage(b)

        return carry

    lax.fori_loop(0, batch + max(off for off, _ in stages), wave, 0)

    def drain(b, carry):
        ref = q_buf.at[b, core, pl.ds(0, 7)]
        remote(ref, ref, q_send.at[b], ql_recv.at[b, 0], partner).wait_send()
        qp_desc(b, core).wait_send()
        d_desc(b).wait_send()
        remote(r_buf.at[b], r_buf.at[b], r_send.at[b], r_recv.at[b, 0], partner).wait_send()
        return carry

    lax.fori_loop(0, batch, drain, 0)


def attention(mesh, q, kv, lengths):
    batch, toks, heads, width = q.shape
    group = mesh.shape['dcp']
    chips = group // 2
    keys = kv.shape[1] * kv.shape[2] * kv.shape[3]
    rows = toks * heads
    bf16 = jnp.bfloat16
    dma = pltpu.SemaphoreType.DMA
    out = pl.pallas_call(
        functools.partial(_kernel, group, toks, heads),
        out_shape=jax.ShapeDtypeStruct((batch, rows, LATENT), bf16),
        in_specs=[
            pl.BlockSpec(memory_space=pltpu.SMEM),
            pl.BlockSpec(memory_space=pl.ANY),
            pl.BlockSpec(memory_space=pl.ANY),
        ],
        out_specs=pl.BlockSpec(memory_space=pltpu.VMEM),
        scratch_shapes=[
            pltpu.VMEM((batch, keys, width), bf16),
            pltpu.VMEM((batch, 2, chips, rows, width), bf16),
            pltpu.VMEM((batch, 2, chips, rows, PACKED), bf16),
            pltpu.VMEM((batch, chips, rows, PACKED), bf16),
            pltpu.VMEM((batch, chips, rows, PACKED), bf16),
            pltpu.VMEM((batch, 7, rows, PACKED), bf16),
            pltpu.VMEM((batch, 5, rows, PACKED), bf16),
            pltpu.VMEM((rows, keys), jnp.int32),
            pltpu.VMEM((group * rows, keys), jnp.float32),
            pltpu.VMEM((group * rows, keys), bf16),
            dma((batch,)),
            dma,
            dma((batch, 7)),
            dma((batch,)),
            dma((batch,)),
            dma((batch,)),
            dma((batch,)),
            dma((batch,)),
            dma((batch, 7)),
            dma((batch,)),
        ],
        compiler_params=pltpu.CompilerParams(collective_id=0, has_side_effects=True, vmem_limit_bytes=60 * 1024 * 1024),
        name='mla_ring',
    )(lengths, q.reshape(batch, rows, width), kv.reshape(batch, keys, width))
    return out.reshape(batch, toks, heads, LATENT)


def solution(mesh):
    return jax.shard_map(
        functools.partial(attention, mesh),
        mesh=mesh,
        in_specs=(P('dp', None, 'dcp', None), P('dp', None, 'dcp', None, None), P('dp')),
        out_specs=P('dp', None, 'dcp', None),
        check_vma=False,
    )
```

```python
import functools
import math

import jax
import jax.numpy as jnp
from jax import lax
from jax.experimental import pallas as pl
from jax.experimental.pallas import tpu as pltpu
from jax.sharding import PartitionSpec as P

LATENT = 512
ROPE = 64
NOPE = 128
PAGE = 64
LANES = 128
PAIR = 2
OUTS = PAIR * LATENT
PACKED = OUTS + LANES
MESH = pl.DeviceIdType.MESH


def _lse_limbs(lses):
    shape = lses[0].shape[:-1] + (LANES,)
    lane = lax.broadcasted_iota(jnp.int32, shape, len(shape) - 1)
    tile = jnp.zeros(shape, jnp.float32)
    for i, lse in enumerate(lses):
        hi = lse.astype(jnp.bfloat16).astype(jnp.float32)
        rest = lse - hi
        mid = rest.astype(jnp.bfloat16).astype(jnp.float32)
        for j, limb in enumerate((hi, mid, rest - mid)):
            tile = jnp.where(lane == 3 * i + j, limb, tile)
    return tile.astype(jnp.bfloat16)


def _merge(parts):
    tails = [p[:, OUTS:].astype(jnp.float32) for p in parts]
    lane = lax.broadcasted_iota(jnp.int32, tails[0].shape, 1)
    outs, lses = [], []
    for i in range(PAIR):
        mine = jnp.logical_and(lane >= 3 * i, lane < 3 * i + 3)
        ls = [jnp.sum(jnp.where(mine, t, 0.0), axis=-1, keepdims=True) for t in tails]
        top = functools.reduce(jnp.maximum, ls)
        ws = [jnp.exp2(x - top) for x in ls]
        total = functools.reduce(jnp.add, ws)
        inv = 1.0 / total
        cols = slice(i * LATENT, (i + 1) * LATENT)
        outs.append(functools.reduce(jnp.add, [p[:, cols].astype(jnp.float32) * (w * inv) for p, w in zip(parts, ws)]))
        lses.append(top + jnp.log2(total))
    return outs, lses


def _pack(outs, lses):
    return [o.astype(jnp.bfloat16) for o in outs] + [_lse_limbs(lses)]


def _kernel(group, toks, heads, len_ref, q_hbm, kv_hbm, o_ref, kv_buf, q_buf, p_buf, d_buf, c_buf, r_buf, s_buf, pos_ref,
            sc_ref, w_ref, st_ref, kv_sem, qin_sem, ql_recv, qp_recv, q_send, qp_send, d_recv, d_send, r_recv, r_send):
    batch, keys, width = kv_buf.shape
    pairs = batch // PAIR
    rows = toks * heads
    chips = group // 2
    all_rows = group * rows
    scale = (NOPE + ROPE) ** -0.5 * math.log2(math.e)
    me = lax.axis_index('dcp')
    z = lax.div(me, 2)
    core = lax.rem(me, 2)
    other = 1 - core
    partner = z * 2 + other

    def chip(off):
        return lax.rem(z + off + chips, chips)

    def dev(off):
        return chip(off) * 2 + core

    def remote(src, dst, send, recv, target):
        return pltpu.make_async_remote_copy(src_ref=src, dst_ref=dst, send_sem=send, recv_sem=recv, device_id={'dcp': target}, device_id_type=MESH)

    def sign(p):
        return 1 - 2 * lax.rem(p, 2)

    def each(lo, hi, stage):
        def step(i, carry):
            stage(i)
            return carry

        lax.fori_loop(lo, hi, step, 0)

    barrier = pltpu.get_barrier_semaphore()
    partners = [dev(off) for off in (-2, -1, 1, 2)] + [partner]
    for target in partners:
        pl.semaphore_signal(barrier, inc=1, device_id={'dcp': target}, device_id_type=MESH)

    own_q = pltpu.make_async_copy(q_hbm, q_buf.at[:, core, z], qin_sem)
    own_q.start()

    def kv_copy(b):
        return pltpu.make_async_copy(kv_hbm.at[b], kv_buf.at[b], kv_sem.at[b])

    each(0, batch, lambda b: kv_copy(b).start())

    col = lax.broadcasted_iota(jnp.int32, (rows, keys), 1)
    tok = lax.broadcasted_iota(jnp.int32, (rows, keys), 0) // heads
    pos_ref[...] = ((col // PAGE) * group + me) * PAGE + col % PAGE - tok + toks

    own_q.wait()
    pl.semaphore_wait(barrier, len(partners))

    def q_desc(p, src, target, slot):
        ref = q_buf.at[p, core, src]
        return remote(ref, ref, q_send.at[p], ql_recv.at[p, slot], target)

    def q0(p):
        q_desc(p, z, dev(1), 0).start()
        q_desc(p, z, dev(-1), 3).start()

    def q1(p):
        q_desc(p, chip(-1), partner, 0).wait_recv()
        q_desc(p, chip(-1), dev(1), 1).start()
        q_desc(p, chip(1), partner, 3).wait_recv()
        q_desc(p, chip(1), dev(-1), 4).start()

    def q2(p):
        q_desc(p, chip(-2), partner, 1).wait_recv()
        q_desc(p, chip(-2), dev(1), 2).start()
        q_desc(p, chip(2), partner, 4).wait_recv()
        q_desc(p, chip(2), dev(-1), 5).start()

    def q3(p):
        q_desc(p, chip(-3), partner, 2).wait_recv()
        q_desc(p, chip(3), partner, 5).wait_recv()
        q_desc(p, chip(-3 * sign(p)), dev(sign(p)), 6).start()

    def qp_desc(p, side):
        ref = q_buf.at[p, side]
        return remote(ref, ref, qp_send.at[p], qp_recv.at[p], partner)

    def q4(p):
        q_desc(p, chip(4), partner, 6).wait_recv()
        qp_desc(p, core).start()

    def d_desc(p):
        return remote(p_buf.at[p, other], d_buf.at[p], d_send.at[p], d_recv.at[p], partner)

    block = 256
    spans = [slice(j, j + block) for j in range(0, keys, block)]

    def scores(p, u):
        q = q_buf[p, :, :, u].reshape(all_rows, width)
        cap = jnp.where(pos_ref[...] <= len_ref[p * PAIR + u], jnp.inf, -jnp.inf).astype(jnp.float32)

        def step(ks):
            s = lax.dot_general(q, kv_buf[p * PAIR + u, ks, :], (((1,), (1,)), ((), ())), preferred_element_type=jnp.float32)
            s = jnp.minimum(s.reshape(group, rows, block) * scale, cap[None, :, ks]).reshape(all_rows, block)
            sc_ref[u, :, ks] = s
            return jnp.max(s, axis=-1, keepdims=True)

        return step

    def weigh(u, top, ks):
        w = jnp.exp2(sc_ref[u, :, ks] - top)
        w_ref[u, :, ks] = w.astype(jnp.bfloat16)
        return jnp.sum(w, axis=-1, keepdims=True)

    def spread(x):
        return jnp.broadcast_to(x, (all_rows, LANES))

    def attend_a(p):
        qp_desc(p, other).wait_recv()
        kv_copy(p * PAIR).wait()
        kv_copy(p * PAIR + 1).wait()
        first, second = scores(p, 0), scores(p, 1)
        top0 = functools.reduce(jnp.maximum, [first(ks) for ks in spans])
        tops, sums = [], []
        for ks in spans:
            tops.append(second(ks))
            sums.append(weigh(0, top0, ks))
        st_ref[0] = spread(top0)
        st_ref[1] = spread(functools.reduce(jnp.maximum, tops))
        st_ref[2] = spread(functools.reduce(jnp.add, sums))

    def attend_b(p):
        def product(u):
            return jnp.dot(w_ref[u], kv_buf[p * PAIR + u, :, :LATENT], preferred_element_type=jnp.float32)

        def keep(u, out, total):
            out = (out * (1.0 / total)).astype(jnp.bfloat16)
            p_buf[p, :, :, :, u * LATENT:(u + 1) * LATENT] = out.reshape(2, chips, rows, LATENT)

        top1 = st_ref[1][:, :1]
        total0 = st_ref[2][:, :1]
        out0 = product(0)
        total1 = functools.reduce(jnp.add, [weigh(1, top1, ks) for ks in spans])
        keep(0, out0, total0)
        tail = _lse_limbs([st_ref[0][:, :1] + jnp.log2(total0), top1 + jnp.log2(total1)])
        p_buf[p, :, :, :, OUTS:] = tail.reshape(2, chips, rows, LANES)
        keep(1, product(1), total1)
        d_desc(p).start()

    def r_desc(p, src, slot, off):
        return remote(src, r_buf.at[p, slot], r_send.at[p], r_recv.at[p, slot], dev(off))

    def r_wait(p, slot):
        r_desc(p, r_buf.at[p, slot], slot, 1).wait_recv()

    cuts = [slice(0, LATENT), slice(LATENT, OUTS), slice(OUTS, PACKED)]

    def o0(p):
        d_desc(p).wait_recv()
        n = chips * rows
        packed = _pack(*_merge([p_buf[p, core].reshape(n, PACKED), d_buf[p].reshape(n, PACKED)]))
        for cut, x in zip(cuts, packed):
            c_buf[p, :, :, cut] = x.reshape(chips, rows, x.shape[-1])
        s = sign(p)
        r_desc(p, c_buf.at[p, chip(4)], 0, 2 * s).start()
        r_desc(p, c_buf.at[p, chip(3 * s)], 1, s).start()
        r_desc(p, c_buf.at[p, chip(-3 * s)], 2, -s).start()
        r_desc(p, c_buf.at[p, chip(1)], 3, 1).start()
        r_desc(p, c_buf.at[p, chip(-1)], 4, -1).start()

    def o1(p):
        s = sign(p)
        for slot in (0, 1, 2):
            r_wait(p, slot)
        far = _pack(*_merge([c_buf[p, chip(2 * s)], r_buf[p, 0], r_buf[p, 1]]))
        near = _pack(*_merge([c_buf[p, chip(-2 * s)], r_buf[p, 2]]))
        for i, packed in enumerate((far, near)):
            for cut, x in zip(cuts, packed):
                s_buf[p, i, :, cut] = x
        r_desc(p, s_buf.at[p, 0], 5, 2 * s).start()
        r_desc(p, s_buf.at[p, 1], 6, -2 * s).start()

    def o2(p):
        for slot in (3, 4, 5, 6):
            r_wait(p, slot)
        outs, _ = _merge([c_buf[p, z]] + [r_buf[p, slot] for slot in (3, 4, 5, 6)])
        for u in range(PAIR):
            o_ref[p, u] = outs[u].astype(jnp.bfloat16)

    for stage in (q0, q1, q2, q3):
        each(0, pairs, stage)
    q4(0)

    stages = [
        (3, o1), (-1, q4), (0, attend_a), (4, o2), (1, o0), (0, attend_b),
    ]

    def wave(w, carry):
        for off, stage in stages:
            p = w - off

            @pl.when(jnp.logical_and(p >= 0, p < pairs))
            def _(stage=stage, p=p):
                stage(p)

        return carry

    lax.fori_loop(0, pairs + max(off for off, _ in stages), wave, 0)

    def drain(p, carry):
        ref = q_buf.at[p, core, pl.ds(0, 7)]
        remote(ref, ref, q_send.at[p], ql_recv.at[p, 0], partner).wait_send()
        qp_desc(p, core).wait_send()
        d_desc(p).wait_send()
        remote(r_buf.at[p], r_buf.at[p], r_send.at[p], r_recv.at[p, 0], partner).wait_send()
        return carry

    lax.fori_loop(0, pairs, drain, 0)


def attention(mesh, q, kv, lengths):
    batch, toks, heads, width = q.shape
    group = mesh.shape['dcp']
    chips = group // 2
    keys = kv.shape[1] * kv.shape[2] * kv.shape[3]
    rows = toks * heads
    pairs = batch // PAIR
    bf16 = jnp.bfloat16
    dma = pltpu.SemaphoreType.DMA
    out = pl.pallas_call(
        functools.partial(_kernel, group, toks, heads),
        out_shape=jax.ShapeDtypeStruct((pairs, PAIR, rows, LATENT), bf16),
        in_specs=[
            pl.BlockSpec(memory_space=pltpu.SMEM),
            pl.BlockSpec(memory_space=pl.ANY),
            pl.BlockSpec(memory_space=pl.ANY),
        ],
        out_specs=pl.BlockSpec(memory_space=pltpu.VMEM),
        scratch_shapes=[
            pltpu.VMEM((batch, keys, width), bf16),
            pltpu.VMEM((pairs, 2, chips, PAIR, rows, width), bf16),
            pltpu.VMEM((pairs, 2, chips, rows, PACKED), bf16),
            pltpu.VMEM((pairs, chips, rows, PACKED), bf16),
            pltpu.VMEM((pairs, chips, rows, PACKED), bf16),
            pltpu.VMEM((pairs, 7, rows, PACKED), bf16),
            pltpu.VMEM((pairs, 2, rows, PACKED), bf16),
            pltpu.VMEM((rows, keys), jnp.int32),
            pltpu.VMEM((PAIR, group * rows, keys), jnp.float32),
            pltpu.VMEM((PAIR, group * rows, keys), bf16),
            pltpu.VMEM((3, group * rows, LANES), jnp.float32),
            dma((batch,)),
            dma,
            dma((pairs, 7)),
            dma((pairs,)),
            dma((pairs,)),
            dma((pairs,)),
            dma((pairs,)),
            dma((pairs,)),
            dma((pairs, 7)),
            dma((pairs,)),
        ],
        compiler_params=pltpu.CompilerParams(collective_id=0, has_side_effects=True, vmem_limit_bytes=60 * 1024 * 1024),
        name='mla_ring',
    )(lengths, q.reshape(pairs, PAIR, rows, width), kv.reshape(batch, keys, width))
    return out.reshape(batch, toks, heads, LATENT)


def solution(mesh):
    return jax.shard_map(
        functools.partial(attention, mesh),
        mesh=mesh,
        in_specs=(P('dp', None, 'dcp', None), P('dp', None, 'dcp', None, None), P('dp')),
        out_specs=P('dp', None, 'dcp', None),
        check_vma=False,
    )
```

```python
import functools
import math

import jax
import jax.numpy as jnp
from jax import lax
from jax.experimental import pallas as pl
from jax.experimental.pallas import tpu as pltpu
from jax.sharding import PartitionSpec as P

LATENT = 512
ROPE = 64
NOPE = 128
PAGE = 64
LANES = 128
PAIR = 2
OUTS = PAIR * LATENT
PACKED = OUTS + LANES
MESH = pl.DeviceIdType.MESH


def _lse_limbs(lses):
    shape = lses[0].shape[:-1] + (LANES,)
    lane = lax.broadcasted_iota(jnp.int32, shape, len(shape) - 1)
    tile = jnp.zeros(shape, jnp.float32)
    for i, lse in enumerate(lses):
        hi = lse.astype(jnp.bfloat16).astype(jnp.float32)
        rest = lse - hi
        mid = rest.astype(jnp.bfloat16).astype(jnp.float32)
        for j, limb in enumerate((hi, mid, rest - mid)):
            tile = jnp.where(lane == 3 * i + j, limb, tile)
    return tile.astype(jnp.bfloat16)


def _merge(parts):
    tails = [p[:, OUTS:].astype(jnp.float32) for p in parts]
    lane = lax.broadcasted_iota(jnp.int32, tails[0].shape, 1)
    outs, lses = [], []
    for i in range(PAIR):
        mine = jnp.logical_and(lane >= 3 * i, lane < 3 * i + 3)
        ls = [jnp.sum(jnp.where(mine, t, 0.0), axis=-1, keepdims=True) for t in tails]
        top = functools.reduce(jnp.maximum, ls)
        ws = [jnp.exp2(x - top) for x in ls]
        total = functools.reduce(jnp.add, ws)
        inv = 1.0 / total
        cols = slice(i * LATENT, (i + 1) * LATENT)
        outs.append(functools.reduce(jnp.add, [p[:, cols].astype(jnp.float32) * (w * inv) for p, w in zip(parts, ws)]))
        lses.append(top + jnp.log2(total))
    return outs, lses


def _pack(outs, lses):
    return [o.astype(jnp.bfloat16) for o in outs] + [_lse_limbs(lses)]


def _kernel(group, toks, heads, len_ref, q_hbm, kv_hbm, o_ref, kv_buf, own_ref, q_buf, p_buf, d_buf, c_buf, r_buf, s_buf, pos_ref,
            sc_ref, w_ref, st_ref, kv_sem, qin_sem, ql_recv, qp_recv, q_send, qp_send, d_recv, d_send, r_recv, r_send):
    batch, keys, width = kv_buf.shape
    pairs = batch // PAIR
    rows = toks * heads
    chips = group // 2
    all_rows = group * rows
    scale = (NOPE + ROPE) ** -0.5 * math.log2(math.e)
    me = lax.axis_index('dcp')
    z = lax.div(me, 2)
    core = lax.rem(me, 2)
    other = 1 - core
    partner = z * 2 + other

    def chip(off):
        return lax.rem(z + off + chips, chips)

    def dev(off):
        return chip(off) * 2 + core

    def remote(src, dst, send, recv, target):
        return pltpu.make_async_remote_copy(src_ref=src, dst_ref=dst, send_sem=send, recv_sem=recv, device_id={'dcp': target}, device_id_type=MESH)

    def sign(p):
        return 1 - 2 * lax.rem(p, 2)

    def each(lo, hi, stage):
        def step(i, carry):
            stage(i)
            return carry

        lax.fori_loop(lo, hi, step, 0)

    barrier = pltpu.get_barrier_semaphore()
    partners = [dev(off) for off in (-2, -1, 1, 2)] + [partner]
    for target in partners:
        pl.semaphore_signal(barrier, inc=1, device_id={'dcp': target}, device_id_type=MESH)

    own_q = pltpu.make_async_copy(q_hbm, own_ref, qin_sem)
    own_q.start()

    def kv_copy(b):
        return pltpu.make_async_copy(kv_hbm.at[b], kv_buf.at[b], kv_sem.at[b])

    each(0, batch, lambda b: kv_copy(b).start())

    col = lax.broadcasted_iota(jnp.int32, (rows, keys), 1)
    tok = lax.broadcasted_iota(jnp.int32, (rows, keys), 0) // heads
    pos_ref[...] = ((col // PAGE) * group + me) * PAGE + col % PAGE - tok + toks

    own_q.wait()
    for p in range(pairs):
        for u in range(PAIR):
            q_buf[p, core, z, :, u * LATENT:(u + 1) * LATENT] = own_ref[p, u, :, :LATENT]
        q_buf[p, core, z, :, OUTS:] = jnp.concatenate([own_ref[p, u, :, LATENT:] for u in range(PAIR)], axis=-1)
    pl.semaphore_wait(barrier, len(partners))

    def q_desc(p, src, target, slot):
        ref = q_buf.at[p, core, src]
        return remote(ref, ref, q_send.at[p], ql_recv.at[p, slot], target)

    def q_far(p):
        q_desc(p, z, dev(2), 1).start()
        q_desc(p, z, dev(-2), 4).start()

    def q_near(p):
        q_desc(p, z, dev(1), 0).start()
        q_desc(p, z, dev(-1), 3).start()

    def q_relay(p):
        q_desc(p, chip(-2), partner, 1).wait_recv()
        q_desc(p, chip(2), partner, 4).wait_recv()
        s = sign(p)
        q_desc(p, chip(-2 * s), dev(2 * s), 6).start()
        q_desc(p, chip(-2), dev(1), 2).start()
        q_desc(p, chip(2), dev(-1), 5).start()

    def qp_desc(p, side):
        ref = q_buf.at[p, side]
        return remote(ref, ref, qp_send.at[p], qp_recv.at[p], partner)

    def q_last(p):
        for off, slot in ((-1, 0), (1, 3), (-3, 2), (3, 5), (4, 6)):
            q_desc(p, chip(off), partner, slot).wait_recv()
        qp_desc(p, core).start()

    def d_desc(p):
        return remote(p_buf.at[p, other], d_buf.at[p], d_send.at[p], d_recv.at[p], partner)

    block = 256
    spans = [slice(j, j + block) for j in range(0, keys, block)]

    def scores(p, u):
        q = jnp.concatenate([
            q_buf[p, :, :, :, u * LATENT:(u + 1) * LATENT].reshape(all_rows, LATENT),
            q_buf[p, :, :, :, OUTS + u * ROPE:OUTS + (u + 1) * ROPE].reshape(all_rows, ROPE),
        ], axis=-1)
        cap = jnp.where(pos_ref[...] <= len_ref[p * PAIR + u], jnp.inf, -jnp.inf).astype(jnp.float32)

        def step(ks):
            s = lax.dot_general(q, kv_buf[p * PAIR + u, ks, :], (((1,), (1,)), ((), ())), preferred_element_type=jnp.float32)
            s = jnp.minimum(s.reshape(group, rows, block) * scale, cap[None, :, ks]).reshape(all_rows, block)
            sc_ref[u, :, ks] = s
            return jnp.max(s, axis=-1, keepdims=True)

        return step

    def weigh(u, top, ks):
        w = jnp.exp2(sc_ref[u, :, ks] - top)
        w_ref[u, :, ks] = w.astype(jnp.bfloat16)
        return jnp.sum(w, axis=-1, keepdims=True)

    def spread(x):
        return jnp.broadcast_to(x, (all_rows, LANES))

    def attend_a(p):
        qp_desc(p, other).wait_recv()
        kv_copy(p * PAIR).wait()
        kv_copy(p * PAIR + 1).wait()
        first, second = scores(p, 0), scores(p, 1)
        top0 = functools.reduce(jnp.maximum, [first(ks) for ks in spans])
        tops, sums = [], []
        for ks in spans:
            tops.append(second(ks))
            sums.append(weigh(0, top0, ks))
        st_ref[0] = spread(top0)
        st_ref[1] = spread(functools.reduce(jnp.maximum, tops))
        st_ref[2] = spread(functools.reduce(jnp.add, sums))

    def attend_b(p):
        def product(u):
            return jnp.dot(w_ref[u], kv_buf[p * PAIR + u, :, :LATENT], preferred_element_type=jnp.float32)

        def keep(u, out, total):
            out = (out * (1.0 / total)).astype(jnp.bfloat16)
            p_buf[p, :, :, :, u * LATENT:(u + 1) * LATENT] = out.reshape(2, chips, rows, LATENT)

        top1 = st_ref[1][:, :1]
        total0 = st_ref[2][:, :1]
        out0 = product(0)
        total1 = functools.reduce(jnp.add, [weigh(1, top1, ks) for ks in spans])
        keep(0, out0, total0)
        tail = _lse_limbs([st_ref[0][:, :1] + jnp.log2(total0), top1 + jnp.log2(total1)])
        p_buf[p, :, :, :, OUTS:] = tail.reshape(2, chips, rows, LANES)
        keep(1, product(1), total1)
        d_desc(p).start()

    def r_desc(p, src, slot, off):
        return remote(src, r_buf.at[p, slot], r_send.at[p], r_recv.at[p, slot], dev(off))

    def r_wait(p, slot):
        r_desc(p, r_buf.at[p, slot], slot, 1).wait_recv()

    cuts = [slice(0, LATENT), slice(LATENT, OUTS), slice(OUTS, PACKED)]

    def o0(p):
        d_desc(p).wait_recv()
        n = chips * rows
        packed = _pack(*_merge([p_buf[p, core].reshape(n, PACKED), d_buf[p].reshape(n, PACKED)]))
        for cut, x in zip(cuts, packed):
            c_buf[p, :, :, cut] = x.reshape(chips, rows, x.shape[-1])
        s = sign(p)
        r_desc(p, c_buf.at[p, chip(4)], 0, 2 * s).start()
        r_desc(p, c_buf.at[p, chip(3 * s)], 1, s).start()
        r_desc(p, c_buf.at[p, chip(-3 * s)], 2, -s).start()
        r_desc(p, c_buf.at[p, chip(1)], 3, 1).start()
        r_desc(p, c_buf.at[p, chip(-1)], 4, -1).start()

    def o1(p):
        s = sign(p)
        for slot in (0, 1, 2):
            r_wait(p, slot)
        far = _pack(*_merge([c_buf[p, chip(2 * s)], r_buf[p, 0], r_buf[p, 1]]))
        near = _pack(*_merge([c_buf[p, chip(-2 * s)], r_buf[p, 2]]))
        for i, packed in enumerate((far, near)):
            for cut, x in zip(cuts, packed):
                s_buf[p, i, :, cut] = x
        r_desc(p, s_buf.at[p, 0], 5, 2 * s).start()
        r_desc(p, s_buf.at[p, 1], 6, -2 * s).start()

    def o2(p):
        for slot in (3, 4, 5, 6):
            r_wait(p, slot)
        outs, _ = _merge([c_buf[p, z]] + [r_buf[p, slot] for slot in (3, 4, 5, 6)])
        for u in range(PAIR):
            o_ref[p, u] = outs[u].astype(jnp.bfloat16)

    for stage, p in ((q_far, 0), (q_near, 0), (q_far, 1), (q_relay, 0), (q_near, 1), (q_far, 2), (q_relay, 1), (q_near, 2), (q_far, 3), (q_last, 0)):
        stage(p)
    late_q = [
        [(0, [(q_last, 1), (q_relay, 2), (q_near, 3)]), (1, [(q_relay, 3)]), (2, [(q_last, 3)])],
        [(2, [(q_last, 2)])],
    ]

    def run(w, todo):
        for at, stage in todo:
            p = w - at

            @pl.when(jnp.logical_and(p >= 0, p < pairs))
            def _(stage=stage, p=p):
                stage(p)

    def run_q(w, todo):
        for at, steps in todo:

            @pl.when(w == at)
            def _(steps=steps):
                for stage, p in steps:
                    stage(p)

    def wave(w, carry):
        run_q(w, late_q[1])
        run(w, [(3, o1), (4, o2), (0, attend_a)])
        run_q(w, late_q[0])
        run(w, [(1, o0), (0, attend_b)])
        return carry

    lax.fori_loop(0, pairs + 4, wave, 0)

    def drain(p, carry):
        ref = q_buf.at[p, core, pl.ds(0, 7)]
        remote(ref, ref, q_send.at[p], ql_recv.at[p, 0], partner).wait_send()
        qp_desc(p, core).wait_send()
        d_desc(p).wait_send()
        remote(r_buf.at[p], r_buf.at[p], r_send.at[p], r_recv.at[p, 0], partner).wait_send()
        return carry

    lax.fori_loop(0, pairs, drain, 0)


def attention(mesh, q, kv, lengths):
    batch, toks, heads, width = q.shape
    group = mesh.shape['dcp']
    chips = group // 2
    keys = kv.shape[1] * kv.shape[2] * kv.shape[3]
    rows = toks * heads
    pairs = batch // PAIR
    bf16 = jnp.bfloat16
    dma = pltpu.SemaphoreType.DMA
    out = pl.pallas_call(
        functools.partial(_kernel, group, toks, heads),
        out_shape=jax.ShapeDtypeStruct((pairs, PAIR, rows, LATENT), bf16),
        in_specs=[
            pl.BlockSpec(memory_space=pltpu.SMEM),
            pl.BlockSpec(memory_space=pl.ANY),
            pl.BlockSpec(memory_space=pl.ANY),
        ],
        out_specs=pl.BlockSpec(memory_space=pltpu.VMEM),
        scratch_shapes=[
            pltpu.VMEM((batch, keys, width), bf16),
            pltpu.VMEM((pairs, PAIR, rows, width), bf16),
            pltpu.VMEM((pairs, 2, chips, rows, PACKED), bf16),
            pltpu.VMEM((pairs, 2, chips, rows, PACKED), bf16),
            pltpu.VMEM((pairs, chips, rows, PACKED), bf16),
            pltpu.VMEM((pairs, chips, rows, PACKED), bf16),
            pltpu.VMEM((pairs, 7, rows, PACKED), bf16),
            pltpu.VMEM((pairs, 2, rows, PACKED), bf16),
            pltpu.VMEM((rows, keys), jnp.int32),
            pltpu.VMEM((PAIR, group * rows, keys), jnp.float32),
            pltpu.VMEM((PAIR, group * rows, keys), bf16),
            pltpu.VMEM((3, group * rows, LANES), jnp.float32),
            dma((batch,)),
            dma,
            dma((pairs, 7)),
            dma((pairs,)),
            dma((pairs,)),
            dma((pairs,)),
            dma((pairs,)),
            dma((pairs,)),
            dma((pairs, 7)),
            dma((pairs,)),
        ],
        compiler_params=pltpu.CompilerParams(collective_id=0, has_side_effects=True, vmem_limit_bytes=60 * 1024 * 1024),
        name='mla_ring',
    )(lengths, q.reshape(pairs, PAIR, rows, width), kv.reshape(batch, keys, width))
    return out.reshape(batch, toks, heads, LATENT)


def solution(mesh):
    return jax.shard_map(
        functools.partial(attention, mesh),
        mesh=mesh,
        in_specs=(P('dp', None, 'dcp', None), P('dp', None, 'dcp', None, None), P('dp')),
        out_specs=P('dp', None, 'dcp', None),
        check_vma=False,
    )
```

```python
import functools
import math
import types

import jax
import jax.numpy as jnp
from jax import lax
from jax.experimental import pallas as pl
from jax.experimental.pallas import tpu as pltpu
from jax.sharding import PartitionSpec as P

LATENT = 512
ROPE = 64
NOPE = 128
PAGE = 64
LANES = 128
UNITS = ((2, 3), (1, 2))
MESH = pl.DeviceIdType.MESH


def _lse_limbs(lses):
    shape = lses[0].shape[:-1] + (LANES,)
    lane = lax.broadcasted_iota(jnp.int32, shape, len(shape) - 1)
    tile = jnp.zeros(shape, jnp.float32)
    for i, lse in enumerate(lses):
        hi = lse.astype(jnp.bfloat16).astype(jnp.float32)
        rest = lse - hi
        mid = rest.astype(jnp.bfloat16).astype(jnp.float32)
        for j, limb in enumerate((hi, mid, rest - mid)):
            tile = jnp.where(lane == 3 * i + j, limb, tile)
    return tile.astype(jnp.bfloat16)


def _merge(parts):
    count = parts[0].shape[1] // LATENT
    tails = [p[:, count * LATENT:].astype(jnp.float32) for p in parts]
    lane = lax.broadcasted_iota(jnp.int32, tails[0].shape, 1)
    outs, lses = [], []
    for i in range(count):
        mine = jnp.logical_and(lane >= 3 * i, lane < 3 * i + 3)
        ls = [jnp.sum(jnp.where(mine, t, 0.0), axis=-1, keepdims=True) for t in tails]
        top = functools.reduce(jnp.maximum, ls)
        ws = [jnp.exp2(x - top) for x in ls]
        total = functools.reduce(jnp.add, ws)
        inv = 1.0 / total
        cols = slice(i * LATENT, (i + 1) * LATENT)
        outs.append(functools.reduce(jnp.add, [p[:, cols].astype(jnp.float32) * (w * inv) for p, w in zip(parts, ws)]))
        lses.append(top + jnp.log2(total))
    return outs, lses


def _pack(outs, lses):
    return [o.astype(jnp.bfloat16) for o in outs] + [_lse_limbs(lses)]


def _kernel(group, toks, heads, len_ref, q_hbm, kv_hbm, o_ref, kv_buf, own_ref, pos_ref, sc_ref, w_ref, st_ref, kv_sem, qin_sem, *sets):
    batch, keys, width = kv_buf.shape
    rows = toks * heads
    chips = group // 2
    all_rows = group * rows
    scale = (NOPE + ROPE) ** -0.5 * math.log2(math.e)
    me = lax.axis_index('dcp')
    z = lax.div(me, 2)
    core = lax.rem(me, 2)
    other = 1 - core
    partner = z * 2 + other

    def chip(off):
        return lax.rem(z + off + chips, chips)

    def dev(off):
        return chip(off) * 2 + core

    def remote(src, dst, send, recv, target):
        return pltpu.make_async_remote_copy(src_ref=src, dst_ref=dst, send_sem=send, recv_sem=recv, device_id={'dcp': target}, device_id_type=MESH)

    def sign(p):
        return 1 - 2 * lax.rem(p, 2)

    def each(lo, hi, stage):
        def step(i, carry):
            stage(i)
            return carry

        lax.fori_loop(lo, hi, step, 0)

    barrier = pltpu.get_barrier_semaphore()
    partners = [dev(off) for off in (-2, -1, 1, 2)] + [partner]
    for target in partners:
        pl.semaphore_signal(barrier, inc=1, device_id={'dcp': target}, device_id_type=MESH)

    own_q = pltpu.make_async_copy(q_hbm, own_ref, qin_sem)
    own_q.start()

    def kv_copy(b):
        return pltpu.make_async_copy(kv_hbm.at[b], kv_buf.at[b], kv_sem.at[b])

    each(0, batch, lambda b: kv_copy(b).start())

    col = lax.broadcasted_iota(jnp.int32, (rows, keys), 1)
    tok = lax.broadcasted_iota(jnp.int32, (rows, keys), 0) // heads
    pos_ref[...] = ((col // PAGE) * group + me) * PAGE + col % PAGE - tok + toks

    own_q.wait()
    block = 256
    spans = [slice(j, j + block) for j in range(0, keys, block)]

    def unit_set(count, units, first, q_buf, p_buf, d_buf, c_buf, r_buf, s_buf, ql_recv, qp_recv, q_send, qp_send, d_recv, d_send, r_recv, r_send):
        outs = count * LATENT
        packed_width = outs + LANES

        def q_pack():
            for p in range(units):
                for u in range(count):
                    q_buf[p, core, z, :, u * LATENT:(u + 1) * LATENT] = own_ref[first + p * count + u, :, :LATENT]
                ropes = [own_ref[first + p * count + u, :, LATENT:] for u in range(count)]
                q_buf[p, core, z, :, outs:outs + count * ROPE] = jnp.concatenate(ropes, axis=-1)
                if count * ROPE < LANES:
                    q_buf[p, core, z, :, outs + count * ROPE:] = jnp.zeros((rows, LANES - count * ROPE), jnp.bfloat16)

        def q_desc(p, src, target, slot):
            ref = q_buf.at[p, core, src]
            return remote(ref, ref, q_send.at[p], ql_recv.at[p, slot], target)

        def q_far(p):
            q_desc(p, z, dev(2), 1).start()
            q_desc(p, z, dev(-2), 4).start()

        def q_near(p):
            q_desc(p, z, dev(1), 0).start()
            q_desc(p, z, dev(-1), 3).start()

        def q_relay(p):
            q_desc(p, chip(-2), partner, 1).wait_recv()
            q_desc(p, chip(2), partner, 4).wait_recv()
            s = sign(p)
            q_desc(p, chip(-2 * s), dev(2 * s), 6).start()
            q_desc(p, chip(-2), dev(1), 2).start()
            q_desc(p, chip(2), dev(-1), 5).start()

        def qp_desc(p, side):
            ref = q_buf.at[p, side]
            return remote(ref, ref, qp_send.at[p], qp_recv.at[p], partner)

        def q_last(p):
            for off, slot in ((-1, 0), (1, 3), (-3, 2), (3, 5), (4, 6)):
                q_desc(p, chip(off), partner, slot).wait_recv()
            qp_desc(p, core).start()

        def d_desc(p):
            return remote(p_buf.at[p, other], d_buf.at[p], d_send.at[p], d_recv.at[p], partner)

        def scores(p, u):
            q = jnp.concatenate([
                q_buf[p, :, :, :, u * LATENT:(u + 1) * LATENT].reshape(all_rows, LATENT),
                q_buf[p, :, :, :, outs + u * ROPE:outs + (u + 1) * ROPE].reshape(all_rows, ROPE),
            ], axis=-1)
            cap = jnp.where(pos_ref[...] <= len_ref[first + p * count + u], jnp.inf, -jnp.inf).astype(jnp.float32)

            def step(ks):
                s = lax.dot_general(q, kv_buf[first + p * count + u, ks, :], (((1,), (1,)), ((), ())), preferred_element_type=jnp.float32)
                s = jnp.minimum(s.reshape(group, rows, block) * scale, cap[None, :, ks]).reshape(all_rows, block)
                sc_ref[u, :, ks] = s
                return jnp.max(s, axis=-1, keepdims=True)

            return step

        def weigh(u, top, ks):
            w = jnp.exp2(sc_ref[u, :, ks] - top)
            w_ref[u, :, ks] = w.astype(jnp.bfloat16)
            return jnp.sum(w, axis=-1, keepdims=True)

        def spread(x):
            return jnp.broadcast_to(x, (all_rows, LANES))

        def attend_a(p):
            qp_desc(p, other).wait_recv()
            for u in range(count):
                kv_copy(first + p * count + u).wait()
            steps = [scores(p, u) for u in range(count)]
            top0 = functools.reduce(jnp.maximum, [steps[0](ks) for ks in spans])
            st_ref[0] = spread(top0)
            if count == 1:
                return
            tops, sums = [], []
            for ks in spans:
                tops.append(steps[1](ks))
                sums.append(weigh(0, top0, ks))
            st_ref[1] = spread(functools.reduce(jnp.maximum, tops))
            st_ref[2] = spread(functools.reduce(jnp.add, sums))

        def attend_b(p):
            def product(u):
                return jnp.dot(w_ref[u], kv_buf[first + p * count + u, :, :LATENT], preferred_element_type=jnp.float32)

            def keep(u, out, total):
                out = (out * (1.0 / total)).astype(jnp.bfloat16)
                p_buf[p, :, :, :, u * LATENT:(u + 1) * LATENT] = out.reshape(2, chips, rows, LATENT)

            def close(tops, totals):
                tail = _lse_limbs([top + jnp.log2(total) for top, total in zip(tops, totals)])
                p_buf[p, :, :, :, outs:] = tail.reshape(2, chips, rows, LANES)

            top0 = st_ref[0][:, :1]
            if count == 1:
                total0 = functools.reduce(jnp.add, [weigh(0, top0, ks) for ks in spans])
                close([top0], [total0])
                keep(0, product(0), total0)
            else:
                top1 = st_ref[1][:, :1]
                total0 = st_ref[2][:, :1]
                out0 = product(0)
                total1 = functools.reduce(jnp.add, [weigh(1, top1, ks) for ks in spans])
                keep(0, out0, total0)
                close([top0, top1], [total0, total1])
                keep(1, product(1), total1)
            d_desc(p).start()

        def r_desc(p, src, slot, off):
            return remote(src, r_buf.at[p, slot], r_send.at[p], r_recv.at[p, slot], dev(off))

        def r_wait(p, slot):
            r_desc(p, r_buf.at[p, slot], slot, 1).wait_recv()

        cuts = [slice(u * LATENT, (u + 1) * LATENT) for u in range(count)] + [slice(outs, packed_width)]

        def o0(p):
            d_desc(p).wait_recv()
            n = chips * rows
            packed = _pack(*_merge([p_buf[p, core].reshape(n, packed_width), d_buf[p].reshape(n, packed_width)]))
            for cut, x in zip(cuts, packed):
                c_buf[p, :, :, cut] = x.reshape(chips, rows, x.shape[-1])
            s = sign(p)
            r_desc(p, c_buf.at[p, chip(4)], 0, 2 * s).start()
            r_desc(p, c_buf.at[p, chip(3 * s)], 1, s).start()
            r_desc(p, c_buf.at[p, chip(-3 * s)], 2, -s).start()
            r_desc(p, c_buf.at[p, chip(1)], 3, 1).start()
            r_desc(p, c_buf.at[p, chip(-1)], 4, -1).start()

        def o1(p):
            s = sign(p)
            for slot in (0, 1, 2):
                r_wait(p, slot)
            far = _pack(*_merge([c_buf[p, chip(2 * s)], r_buf[p, 0], r_buf[p, 1]]))
            near = _pack(*_merge([c_buf[p, chip(-2 * s)], r_buf[p, 2]]))
            for i, packed in enumerate((far, near)):
                for cut, x in zip(cuts, packed):
                    s_buf[p, i, :, cut] = x
            r_desc(p, s_buf.at[p, 0], 5, 2 * s).start()
            r_desc(p, s_buf.at[p, 1], 6, -2 * s).start()

        def o2(p):
            for slot in (3, 4, 5, 6):
                r_wait(p, slot)
            merged, _ = _merge([c_buf[p, z]] + [r_buf[p, slot] for slot in (3, 4, 5, 6)])
            for u in range(count):
                o_ref[first + p * count + u] = merged[u].astype(jnp.bfloat16)

        def drain(p):
            ref = q_buf.at[p, core, pl.ds(0, 7)]
            remote(ref, ref, q_send.at[p], ql_recv.at[p, 0], partner).wait_send()
            qp_desc(p, core).wait_send()
            d_desc(p).wait_send()
            remote(r_buf.at[p], r_buf.at[p], r_send.at[p], r_recv.at[p, 0], partner).wait_send()

        return types.SimpleNamespace(
            pack=q_pack, far=q_far, near=q_near, relay=q_relay, last=q_last, attend_a=attend_a, attend_b=attend_b,
            o0=o0, o1=o1, o2=o2, drain=drain,
        )

    size = len(sets) // len(UNITS)
    built, start = [], 0
    for i, (count, units) in enumerate(UNITS):
        built.append(unit_set(count, units, start, *sets[i * size:(i + 1) * size]))
        start += count * units
    two, one = built
    two.pack()
    one.pack()
    pl.semaphore_wait(barrier, len(partners))

    two.far(0)
    two.near(0)
    two.far(1)
    two.relay(0)
    two.near(1)
    two.far(2)
    two.relay(1)
    two.near(2)
    one.far(0)
    one.far(1)
    two.last(0)

    def when(w, lo, hi, stage, p):
        @pl.when(jnp.logical_and(w >= lo, w < hi))
        def _():
            stage(p)

    def wave(w, carry):
        two.attend_a(w)

        @pl.when(w == 0)
        def _():
            two.last(1)
            two.relay(2)
            one.near(0)
            one.near(1)

        @pl.when(w == 1)
        def _():
            two.last(2)
            one.relay(0)
            one.relay(1)

        when(w, 2, 3, one.last, 0)
        when(w, 1, 3, two.o0, w - 1)
        two.attend_b(w)
        return carry

    lax.fori_loop(0, UNITS[0][1], wave, 0)
    two.o1(0)
    one.attend_a(0)
    one.last(1)
    two.o0(2)
    one.attend_b(0)
    two.o1(1)
    one.attend_a(1)
    one.o0(0)
    one.attend_b(1)
    one.o0(1)
    two.o2(0)
    two.o1(2)
    one.o1(0)
    one.o1(1)
    two.o2(1)
    two.o2(2)
    one.o2(0)
    one.o2(1)
    each(0, UNITS[0][1], two.drain)
    each(0, UNITS[1][1], one.drain)


def attention(mesh, q, kv, lengths):
    batch, toks, heads, width = q.shape
    group = mesh.shape['dcp']
    chips = group // 2
    keys = kv.shape[1] * kv.shape[2] * kv.shape[3]
    rows = toks * heads
    bf16 = jnp.bfloat16
    dma = pltpu.SemaphoreType.DMA
    sets = []
    for count, units in UNITS:
        packed = count * LATENT + LANES
        sets += [
            pltpu.VMEM((units, 2, chips, rows, packed), bf16),
            pltpu.VMEM((units, 2, chips, rows, packed), bf16),
            pltpu.VMEM((units, chips, rows, packed), bf16),
            pltpu.VMEM((units, chips, rows, packed), bf16),
            pltpu.VMEM((units, 7, rows, packed), bf16),
            pltpu.VMEM((units, 2, rows, packed), bf16),
            dma((units, 7)),
            dma((units,)),
            dma((units,)),
            dma((units,)),
            dma((units,)),
            dma((units,)),
            dma((units, 7)),
            dma((units,)),
        ]
    out = pl.pallas_call(
        functools.partial(_kernel, group, toks, heads),
        out_shape=jax.ShapeDtypeStruct((batch, rows, LATENT), bf16),
        in_specs=[
            pl.BlockSpec(memory_space=pltpu.SMEM),
            pl.BlockSpec(memory_space=pl.ANY),
            pl.BlockSpec(memory_space=pl.ANY),
        ],
        out_specs=pl.BlockSpec(memory_space=pltpu.VMEM),
        scratch_shapes=[
            pltpu.VMEM((batch, keys, width), bf16),
            pltpu.VMEM((batch, rows, width), bf16),
            pltpu.VMEM((rows, keys), jnp.int32),
            pltpu.VMEM((2, group * rows, keys), jnp.float32),
            pltpu.VMEM((2, group * rows, keys), bf16),
            pltpu.VMEM((3, group * rows, LANES), jnp.float32),
            dma((batch,)),
            dma,
        ] + sets,
        compiler_params=pltpu.CompilerParams(collective_id=0, has_side_effects=True, vmem_limit_bytes=60 * 1024 * 1024),
        name='mla_ring',
    )(lengths, q.reshape(batch, rows, width), kv.reshape(batch, keys, width))
    return out.reshape(batch, toks, heads, LATENT)


def solution(mesh):
    return jax.shard_map(
        functools.partial(attention, mesh),
        mesh=mesh,
        in_specs=(P('dp', None, 'dcp', None), P('dp', None, 'dcp', None, None), P('dp')),
        out_specs=P('dp', None, 'dcp', None),
        check_vma=False,
    )
```

```python
import functools
import math
import types

import jax
import jax.numpy as jnp
from jax import lax
from jax.experimental import pallas as pl
from jax.experimental.pallas import tpu as pltpu
from jax.sharding import PartitionSpec as P

LATENT = 512
ROPE = 64
NOPE = 128
PAGE = 64
LANES = 128
UNITS = ((2, 3), (1, 2))
MESH = pl.DeviceIdType.MESH


def _lse_limbs(lses):
    shape = lses[0].shape[:-1] + (LANES,)
    lane = lax.broadcasted_iota(jnp.int32, shape, len(shape) - 1)
    tile = jnp.zeros(shape, jnp.float32)
    for i, lse in enumerate(lses):
        hi = lse.astype(jnp.bfloat16).astype(jnp.float32)
        rest = lse - hi
        mid = rest.astype(jnp.bfloat16).astype(jnp.float32)
        for j, limb in enumerate((hi, mid, rest - mid)):
            tile = jnp.where(lane == 3 * i + j, limb, tile)
    return tile.astype(jnp.bfloat16)


def _merge(parts):
    count = parts[0].shape[1] // LATENT
    tails = [p[:, count * LATENT:].astype(jnp.float32) for p in parts]
    lane = lax.broadcasted_iota(jnp.int32, tails[0].shape, 1)
    outs, lses = [], []
    for i in range(count):
        mine = jnp.logical_and(lane >= 3 * i, lane < 3 * i + 3)
        ls = [jnp.sum(jnp.where(mine, t, 0.0), axis=-1, keepdims=True) for t in tails]
        top = functools.reduce(jnp.maximum, ls)
        ws = [jnp.exp2(x - top) for x in ls]
        total = functools.reduce(jnp.add, ws)
        inv = 1.0 / total
        cols = slice(i * LATENT, (i + 1) * LATENT)
        outs.append(functools.reduce(jnp.add, [p[:, cols].astype(jnp.float32) * (w * inv) for p, w in zip(parts, ws)]))
        lses.append(top + jnp.log2(total))
    return outs, lses


def _pack(outs, lses):
    return [o.astype(jnp.bfloat16) for o in outs] + [_lse_limbs(lses)]


def _kernel(group, toks, heads, len_ref, q_hbm, kv_hbm, o_hbm, o_ref, out_sem, kv_buf, own_ref, pos_ref, sc_ref, w_ref, st_ref, kv_sem, qin_sem, *sets):
    batch, keys, width = kv_buf.shape
    rows = toks * heads
    chips = group // 2
    all_rows = group * rows
    scale = (NOPE + ROPE) ** -0.5 * math.log2(math.e)
    me = lax.axis_index('dcp')
    z = lax.div(me, 2)
    core = lax.rem(me, 2)
    other = 1 - core
    partner = z * 2 + other

    def chip(off):
        return lax.rem(z + off + chips, chips)

    def dev(off):
        return chip(off) * 2 + core

    def remote(src, dst, send, recv, target):
        return pltpu.make_async_remote_copy(src_ref=src, dst_ref=dst, send_sem=send, recv_sem=recv, device_id={'dcp': target}, device_id_type=MESH)

    def sign(p):
        return 1 - 2 * lax.rem(p, 2)

    def each(lo, hi, stage):
        def step(i, carry):
            stage(i)
            return carry

        lax.fori_loop(lo, hi, step, 0)

    barrier = pltpu.get_barrier_semaphore()
    partners = [dev(off) for off in (-2, -1, 1, 2)] + [partner]
    for target in partners:
        pl.semaphore_signal(barrier, inc=1, device_id={'dcp': target}, device_id_type=MESH)

    own_q = pltpu.make_async_copy(q_hbm, own_ref, qin_sem)
    own_q.start()

    def kv_copy(b):
        return pltpu.make_async_copy(kv_hbm.at[b], kv_buf.at[b], kv_sem.at[b])

    each(0, batch, lambda b: kv_copy(b).start())

    def out_copy(b):
        return pltpu.make_async_copy(o_ref.at[b], o_hbm.at[b], out_sem.at[b])

    col = lax.broadcasted_iota(jnp.int32, (rows, keys), 1)
    tok = lax.broadcasted_iota(jnp.int32, (rows, keys), 0) // heads
    pos_ref[...] = ((col // PAGE) * group + me) * PAGE + col % PAGE - tok + toks

    own_q.wait()
    block = 256
    spans = [slice(j, j + block) for j in range(0, keys, block)]

    def unit_set(count, units, first, q_buf, p_buf, d_buf, c_buf, r_buf, s_buf, ql_recv, qp_recv, q_send, qp_send, d_recv, d_send, r_recv, r_send):
        outs = count * LATENT
        packed_width = outs + LANES

        def q_pack():
            for p in range(units):
                for u in range(count):
                    q_buf[p, core, z, :, u * LATENT:(u + 1) * LATENT] = own_ref[first + p * count + u, :, :LATENT]
                ropes = [own_ref[first + p * count + u, :, LATENT:] for u in range(count)]
                q_buf[p, core, z, :, outs:outs + count * ROPE] = jnp.concatenate(ropes, axis=-1)
                if count * ROPE < LANES:
                    q_buf[p, core, z, :, outs + count * ROPE:] = jnp.zeros((rows, LANES - count * ROPE), jnp.bfloat16)

        def q_desc(p, src, target, slot):
            ref = q_buf.at[p, core, src]
            return remote(ref, ref, q_send.at[p], ql_recv.at[p, slot], target)

        def q_far(p):
            q_desc(p, z, dev(2), 1).start()
            q_desc(p, z, dev(-2), 4).start()

        def q_near(p):
            q_desc(p, z, dev(1), 0).start()
            q_desc(p, z, dev(-1), 3).start()

        def q_relay(p):
            q_desc(p, chip(-2), partner, 1).wait_recv()
            q_desc(p, chip(2), partner, 4).wait_recv()
            s = sign(p)
            q_desc(p, chip(-2 * s), dev(2 * s), 6).start()
            q_desc(p, chip(-2), dev(1), 2).start()
            q_desc(p, chip(2), dev(-1), 5).start()

        def qp_desc(p, side):
            ref = q_buf.at[p, side]
            return remote(ref, ref, qp_send.at[p], qp_recv.at[p], partner)

        def q_last(p):
            for off, slot in ((-1, 0), (1, 3), (-3, 2), (3, 5), (4, 6)):
                q_desc(p, chip(off), partner, slot).wait_recv()
            qp_desc(p, core).start()

        def d_desc(p):
            return remote(p_buf.at[p, other], d_buf.at[p], d_send.at[p], d_recv.at[p], partner)

        def scores(p, u):
            q = jnp.concatenate([
                q_buf[p, :, :, :, u * LATENT:(u + 1) * LATENT].reshape(all_rows, LATENT),
                q_buf[p, :, :, :, outs + u * ROPE:outs + (u + 1) * ROPE].reshape(all_rows, ROPE),
            ], axis=-1)
            cap = jnp.where(pos_ref[...] <= len_ref[first + p * count + u], jnp.inf, -jnp.inf).astype(jnp.float32)

            def step(ks):
                s = lax.dot_general(q, kv_buf[first + p * count + u, ks, :], (((1,), (1,)), ((), ())), preferred_element_type=jnp.float32)
                s = jnp.minimum(s.reshape(group, rows, block) * scale, cap[None, :, ks]).reshape(all_rows, block)
                sc_ref[u, :, ks] = s
                return jnp.max(s, axis=-1, keepdims=True)

            return step

        def weigh(u, top, ks):
            w = jnp.exp2(sc_ref[u, :, ks] - top)
            w_ref[u, :, ks] = w.astype(jnp.bfloat16)
            return jnp.sum(w, axis=-1, keepdims=True)

        def spread(x):
            return jnp.broadcast_to(x, (all_rows, LANES))

        def attend_a(p):
            qp_desc(p, other).wait_recv()
            for u in range(count):
                kv_copy(first + p * count + u).wait()
            steps = [scores(p, u) for u in range(count)]
            top0 = functools.reduce(jnp.maximum, [steps[0](ks) for ks in spans])
            st_ref[0] = spread(top0)
            if count == 1:
                return
            tops, sums = [], []
            for ks in spans:
                tops.append(steps[1](ks))
                sums.append(weigh(0, top0, ks))
            st_ref[1] = spread(functools.reduce(jnp.maximum, tops))
            st_ref[2] = spread(functools.reduce(jnp.add, sums))

        def attend_b(p):
            def product(u):
                return jnp.dot(w_ref[u], kv_buf[first + p * count + u, :, :LATENT], preferred_element_type=jnp.float32)

            def keep(u, out, total):
                out = (out * (1.0 / total)).astype(jnp.bfloat16)
                p_buf[p, :, :, :, u * LATENT:(u + 1) * LATENT] = out.reshape(2, chips, rows, LATENT)

            def close(tops, totals):
                tail = _lse_limbs([top + jnp.log2(total) for top, total in zip(tops, totals)])
                p_buf[p, :, :, :, outs:] = tail.reshape(2, chips, rows, LANES)

            top0 = st_ref[0][:, :1]
            if count == 1:
                total0 = functools.reduce(jnp.add, [weigh(0, top0, ks) for ks in spans])
                close([top0], [total0])
                keep(0, product(0), total0)
            else:
                top1 = st_ref[1][:, :1]
                total0 = st_ref[2][:, :1]
                out0 = product(0)
                total1 = functools.reduce(jnp.add, [weigh(1, top1, ks) for ks in spans])
                keep(0, out0, total0)
                close([top0, top1], [total0, total1])
                keep(1, product(1), total1)
            d_desc(p).start()

        def r_desc(p, src, slot, off):
            return remote(src, r_buf.at[p, slot], r_send.at[p], r_recv.at[p, slot], dev(off))

        def r_wait(p, slot):
            r_desc(p, r_buf.at[p, slot], slot, 1).wait_recv()

        cuts = [slice(u * LATENT, (u + 1) * LATENT) for u in range(count)] + [slice(outs, packed_width)]

        def o0(p):
            d_desc(p).wait_recv()
            n = chips * rows
            packed = _pack(*_merge([p_buf[p, core].reshape(n, packed_width), d_buf[p].reshape(n, packed_width)]))
            for cut, x in zip(cuts, packed):
                c_buf[p, :, :, cut] = x.reshape(chips, rows, x.shape[-1])
            s = sign(p)
            r_desc(p, c_buf.at[p, chip(4)], 0, 2 * s).start()
            r_desc(p, c_buf.at[p, chip(3 * s)], 1, s).start()
            r_desc(p, c_buf.at[p, chip(-3 * s)], 2, -s).start()
            r_desc(p, c_buf.at[p, chip(1)], 3, 1).start()
            r_desc(p, c_buf.at[p, chip(-1)], 4, -1).start()

        def o1(p):
            s = sign(p)
            for slot in (0, 1, 2):
                r_wait(p, slot)
            far = _pack(*_merge([c_buf[p, chip(2 * s)], r_buf[p, 0], r_buf[p, 1]]))
            near = _pack(*_merge([c_buf[p, chip(-2 * s)], r_buf[p, 2]]))
            for i, packed in enumerate((far, near)):
                for cut, x in zip(cuts, packed):
                    s_buf[p, i, :, cut] = x
            r_desc(p, s_buf.at[p, 0], 5, 2 * s).start()
            r_desc(p, s_buf.at[p, 1], 6, -2 * s).start()

        def o2(p):
            for slot in (3, 4, 5, 6):
                r_wait(p, slot)
            merged, _ = _merge([c_buf[p, z]] + [r_buf[p, slot] for slot in (3, 4, 5, 6)])
            for u in range(count):
                o_ref[first + p * count + u] = merged[u].astype(jnp.bfloat16)
                out_copy(first + p * count + u).start()

        def drain(p):
            ref = q_buf.at[p, core, pl.ds(0, 7)]
            remote(ref, ref, q_send.at[p], ql_recv.at[p, 0], partner).wait_send()
            qp_desc(p, core).wait_send()
            d_desc(p).wait_send()
            remote(r_buf.at[p], r_buf.at[p], r_send.at[p], r_recv.at[p, 0], partner).wait_send()

        return types.SimpleNamespace(
            pack=q_pack, far=q_far, near=q_near, relay=q_relay, last=q_last, attend_a=attend_a, attend_b=attend_b,
            o0=o0, o1=o1, o2=o2, drain=drain,
        )

    size = len(sets) // len(UNITS)
    built, start = [], 0
    for i, (count, units) in enumerate(UNITS):
        built.append(unit_set(count, units, start, *sets[i * size:(i + 1) * size]))
        start += count * units
    two, one = built
    two.pack()
    one.pack()
    pl.semaphore_wait(barrier, len(partners))

    two.far(0)
    two.near(0)
    two.far(1)
    two.relay(0)
    two.near(1)
    two.far(2)
    two.relay(1)
    two.near(2)
    one.far(0)
    one.far(1)
    two.last(0)

    def when(w, lo, hi, stage, p):
        @pl.when(jnp.logical_and(w >= lo, w < hi))
        def _():
            stage(p)

    def wave(w, carry):
        two.attend_a(w)

        @pl.when(w == 0)
        def _():
            two.last(1)
            two.relay(2)
            one.near(0)
            one.near(1)

        @pl.when(w == 1)
        def _():
            two.last(2)
            one.relay(0)
            one.relay(1)

        when(w, 2, 3, one.last, 0)
        when(w, 1, 3, two.o0, w - 1)
        two.attend_b(w)
        return carry

    lax.fori_loop(0, UNITS[0][1], wave, 0)
    two.o1(0)
    one.attend_a(0)
    one.last(1)
    two.o0(2)
    one.attend_b(0)
    two.o1(1)
    one.attend_a(1)
    one.o0(0)
    one.attend_b(1)
    one.o0(1)
    two.o2(0)
    two.o1(2)
    one.o1(0)
    one.o1(1)
    two.o2(1)
    two.o2(2)
    one.o2(0)
    one.o2(1)
    each(0, UNITS[0][1], two.drain)
    each(0, UNITS[1][1], one.drain)
    each(0, batch, lambda b: out_copy(b).wait())


def attention(mesh, q, kv, lengths):
    batch, toks, heads, width = q.shape
    group = mesh.shape['dcp']
    chips = group // 2
    keys = kv.shape[1] * kv.shape[2] * kv.shape[3]
    rows = toks * heads
    bf16 = jnp.bfloat16
    dma = pltpu.SemaphoreType.DMA
    sets = []
    for count, units in UNITS:
        packed = count * LATENT + LANES
        sets += [
            pltpu.VMEM((units, 2, chips, rows, packed), bf16),
            pltpu.VMEM((units, 2, chips, rows, packed), bf16),
            pltpu.VMEM((units, chips, rows, packed), bf16),
            pltpu.VMEM((units, chips, rows, packed), bf16),
            pltpu.VMEM((units, 7, rows, packed), bf16),
            pltpu.VMEM((units, 2, rows, packed), bf16),
            dma((units, 7)),
            dma((units,)),
            dma((units,)),
            dma((units,)),
            dma((units,)),
            dma((units,)),
            dma((units, 7)),
            dma((units,)),
        ]
    out = pl.pallas_call(
        functools.partial(_kernel, group, toks, heads),
        out_shape=jax.ShapeDtypeStruct((batch, rows, LATENT), bf16),
        in_specs=[
            pl.BlockSpec(memory_space=pltpu.SMEM),
            pl.BlockSpec(memory_space=pl.ANY),
            pl.BlockSpec(memory_space=pl.ANY),
        ],
        out_specs=pl.BlockSpec(memory_space=pl.ANY),
        scratch_shapes=[
            pltpu.VMEM((batch, rows, LATENT), bf16),
            dma((batch,)),
            pltpu.VMEM((batch, keys, width), bf16),
            pltpu.VMEM((batch, rows, width), bf16),
            pltpu.VMEM((rows, keys), jnp.int32),
            pltpu.VMEM((2, group * rows, keys), jnp.float32),
            pltpu.VMEM((2, group * rows, keys), bf16),
            pltpu.VMEM((3, group * rows, LANES), jnp.float32),
            dma((batch,)),
            dma,
        ] + sets,
        compiler_params=pltpu.CompilerParams(collective_id=0, has_side_effects=True, vmem_limit_bytes=60 * 1024 * 1024),
        name='mla_ring',
    )(lengths, q.reshape(batch, rows, width), kv.reshape(batch, keys, width))
    return out.reshape(batch, toks, heads, LATENT)


def solution(mesh):
    return jax.shard_map(
        functools.partial(attention, mesh),
        mesh=mesh,
        in_specs=(P('dp', None, 'dcp', None), P('dp', None, 'dcp', None, None), P('dp')),
        out_specs=P('dp', None, 'dcp', None),
        check_vma=False,
    )
```
